8 devices in a mesh: dp: 1 (over z), ep: 8 (over x, y, core).
Axes of the slice: x: 2, y: 2, z: 1, core: 2. Of those that a mesh axis runs over, the one named last changes fastest.
Arguments:
- x: bfloat16 [1, 8, 256, 4096], P('dp', 'ep')
- expert: int32 [1, 8, 256, 8], P('dp', 'ep')
- slot: int32 [1, 8, 256, 8], P('dp', 'ep')
- gate: float32 [1, 8, 256, 8], P('dp', 'ep')
- w_gate: bfloat16 [64, 4096, 1408], P('ep')
- w_up: bfloat16 [64, 4096, 1408], P('ep')
- w_down: bfloat16 [64, 1408, 4096], P('ep')
- s_gate: bfloat16 [4096, 1408], replicated
- s_up: bfloat16 [4096, 1408], replicated
- s_down: bfloat16 [1408, 4096], replicated
Outputs:
- y: bfloat16 [1, 8, 256, 4096], P('dp', 'ep')
All inputs are finite; a program needn't handle non-finite values.
Results may differ from the reference program's by a relative error of at most 0.009.
Values are sent between devices in bfloat16 or wider.
A program may use at most 2 GiB of HBM per device.

```python
import jax
import jax.numpy as jnp

MEMBERS = 8
TOKENS = 256
D = 4096
FF = 1408
TOP = 8
EXPERTS = 64
SHARED_FF = 1408
SLOTS = 5 * TOKENS * TOP // (4 * EXPERTS)


def setup_inputs(seed: int = 0, part: int = 0) -> dict:
    own, k1, k2, k3, k4, k5, k6 = jax.random.split(jax.random.key(seed), 7)
    kx, ke, kl, kg = jax.random.split(jax.random.fold_in(own, part), 4)
    devices = (1, MEMBERS)
    place = jax.random.permutation(kl, jnp.arange(EXPERTS, dtype=jnp.uint32))
    slow = ((EXPERTS + (9 * place) % EXPERTS) << ((9 * place) // EXPERTS)) // EXPERTS
    wait = (jax.random.bits(ke, (*devices, TOKENS, EXPERTS), jnp.uint32) >> 10) * slow
    expert = jnp.argsort(wait, axis=-1)[..., :TOP].astype(jnp.int32)
    chosen = jax.nn.one_hot(expert, EXPERTS, dtype=jnp.int32)
    in_line = jnp.cumsum(chosen.reshape(*devices, TOKENS * TOP, EXPERTS), axis=2) - 1
    slot = jnp.sum(in_line.reshape(chosen.shape) * chosen, axis=-1)

    def one(key, rows, columns):
        return (jax.random.normal(key, (rows, columns), jnp.float32) * rows**-0.5).astype(jnp.bfloat16)

    def weights(key, rows, columns):
        return jax.lax.map(lambda k: one(k, rows, columns), jax.random.split(key, EXPERTS))

    return {
        "x": jax.random.normal(kx, (*devices, TOKENS, D), jnp.float32).astype(jnp.bfloat16),
        "expert": expert,
        "slot": slot,
        "gate": jax.nn.softmax(jax.random.normal(kg, expert.shape, jnp.float32)),
        "w_gate": weights(k1, D, FF),
        "w_up": weights(k2, D, FF),
        "w_down": weights(k3, FF, D),
        "s_gate": one(k4, D, SHARED_FF),
        "s_up": one(k5, D, SHARED_FF),
        "s_down": one(k6, SHARED_FF, D),
    }


def einsum(form, a, b):
    return jnp.einsum(form, a.astype(jnp.float32), b.astype(jnp.float32))


def for_all(x, s_gate, s_up, s_down):
    h = jax.nn.silu(einsum("...d,df->...f", x, s_gate)) * einsum("...d,df->...f", x, s_up)
    return einsum("...f,fd->...d", h.astype(jnp.bfloat16), s_down)


def reference(x, expert, slot, gate, w_gate, w_up, w_down, s_gate, s_up, s_down):
    to_expert = jax.nn.one_hot(expert, EXPERTS, dtype=jnp.bfloat16)
    to_slot = jax.nn.one_hot(slot, SLOTS, dtype=jnp.bfloat16)
    weighted = to_expert * gate[..., None].astype(jnp.bfloat16)
    dispatch = einsum("abtke,abtkc->abtec", to_expert, to_slot).astype(jnp.bfloat16)
    combine = einsum("abtke,abtkc->abtec", weighted, to_slot).astype(jnp.bfloat16)
    z = einsum("abtec,abtd->aebcd", dispatch, x).astype(jnp.bfloat16)
    h = jax.nn.silu(einsum("aebcd,edf->aebcf", z, w_gate))
    h = (h * einsum("aebcd,edf->aebcf", z, w_up)).astype(jnp.bfloat16)
    out = einsum("aebcf,efd->aebcd", h, w_down).astype(jnp.bfloat16)
    y = einsum("abtec,aebcd->abtd", combine, out)
    return (y + for_all(x, s_gate, s_up, s_down)).astype(jnp.bfloat16)
```

```python
import functools

import jax
import jax.numpy as jnp
from jax import lax
from jax.experimental import pallas as pl
from jax.experimental.pallas import tpu as pltpu
from jax.sharding import PartitionSpec as P

N = 8
T = 256
D = 4096
FF = 1408
EL = 8
SL = 40
R = EL * SL
EM = N * SL
ROWS = EL * EM
W = 256
KC = 512
NC = D // KC
NS = D // W
NT = 2 * FF // W
KT = 6
SLOT = 5632
NSLOT = 3
ITEMS1 = NC + NC * EL
PER2 = 5
ITEMS = ITEMS1 + NC * PER2

S1R = KT * ROWS
S2R = S1R + NC * 512
SIBR = S2R + NC * 1024
S1S = SIBR + 2 * 2048
XROWS = S1S + 2 * 512
YST = 2048
SHR = NC * 2048

f32, bf16 = jnp.float32, jnp.bfloat16


def dot(a, b):
    return jnp.dot(a, b, preferred_element_type=f32)


def kernel(x, info, wg, wu, wd, sg, su, sd, y, xbuf, acc, w, z, dm, cm, hsh, ssend, infos,
           wsem, xsem, is_, ir, ag_s, xy_r, dg_r, sb_r, sib_s, sib_r, s1_s, s1_r, s2_s, s2_r, ysem, credit, ready):
    me = lax.axis_index("ep")
    mx, my, mc = me // 4, (me // 2) % 2, me % 2
    dx = (1 - mx) * 4 + my * 2 + mc
    dy = mx * 4 + (1 - my) * 2 + mc
    dd = (1 - mx) * 4 + (1 - my) * 2 + mc
    ds = mx * 4 + my * 2 + (1 - mc)

    def rows(ref, start, n):
        return ref.at[pl.ds(pl.multiple_of(start, 8), n)]

    def ld(ref, start, n):
        return ref[pl.ds(pl.multiple_of(start, 8), n), :]

    def send(src, dst, ss, rs, dev):
        pltpu.make_async_remote_copy(
            src_ref=src, dst_ref=dst, send_sem=ss, recv_sem=rs,
            device_id={"ep": dev}, device_id_type=pl.DeviceIdType.MESH).start()

    def wait(ref, n, sem):
        v = ref.at[pl.ds(0, n)]
        pltpu.make_async_copy(v, v, sem).wait()

    def start_item(i):
        slot = i % NSLOT
        base = slot * SLOT
        sem = wsem.at[slot]

        def first(g, u, c):
            def put(src, c0, n, t, l0):
                pltpu.make_async_copy(
                    src.at[pl.ds(pl.multiple_of(c * KC, KC), KC), pl.ds(c0, n)],
                    w.at[pl.ds(pl.multiple_of(base + t * KC, KC), KC), pl.ds(l0, n)], sem).start()
            for t in range(5):
                put(g, t * W, W, t, 0)
            put(g, 5 * W, 128, 5, 0)
            put(u, 5 * W, 128, 5, 128)
            for t in range(5):
                put(u, t * W, W, 6 + t, 0)

        @pl.when(i < NC)
        def _():
            first(sg, su, i)

        @pl.when((i >= NC) & (i < ITEMS1))
        def _():
            k = i - NC
            first(wg.at[k % EL], wu.at[k % EL], k // EL)

        @pl.when((i >= ITEMS1) & (i < ITEMS))
        def _():
            k = i - ITEMS1
            c, j = k // PER2, k % PER2

            def put(src, h, t):
                pltpu.make_async_copy(
                    src.at[:, pl.ds(pl.multiple_of(c * KC + h * W, W), W)],
                    rows(w, base + t * FF, FF), sem).start()

            @pl.when(j < 4)
            def _():
                for ee in range(2):
                    for h in range(2):
                        put(wd.at[j * 2 + ee], h, ee * 2 + h)

            @pl.when(j == 4)
            def _():
                for h in range(2):
                    put(sd, h, h)

    def wait_item(i, n=SLOT):
        wait(w, n, wsem.at[i % NSLOT])
        return (i % NSLOT) * SLOT

    def xr(s, src, r0=0, n=T):
        return rows(xbuf, (s * N + src) * T + r0, n)

    def own_out(s):
        for dev, sem in ((dx, xy_r), (dy, xy_r), (ds, sb_r)):
            send(xr(s, me), xr(s, me), ag_s.at[s], sem.at[s], dev)

    def tick(k):
        @pl.when(k < NS)
        def _():
            wait(xbuf, 2 * T, xy_r.at[k])
            send(xr(k, dx, 0, 128), xr(k, dx, 0, 128), ag_s.at[k], dg_r.at[k], dy)
            send(xr(k, dy, 128, 128), xr(k, dy, 128, 128), ag_s.at[k], dg_r.at[k], dx)
            send(xr(k, dx), xr(k, dx), ag_s.at[k], sb_r.at[k], ds)
            send(xr(k, dy), xr(k, dy), ag_s.at[k], sb_r.at[k], ds)

        @pl.when(k + 2 < NS)
        def _():
            own_out(k + 2)

        @pl.when((k >= 1) & (k <= NS))
        def _():
            wait(xbuf, T, dg_r.at[k - 1])
            send(xr(k - 1, dd), xr(k - 1, dd), ag_s.at[k - 1], sb_r.at[k - 1], ds)

    for s in range(NS):
        pltpu.make_async_copy(x.at[:, pl.ds(s * W, W)], xr(s, me), xsem).start()
    for i in range(NSLOT):
        start_item(jnp.int32(i))
    barrier = pltpu.get_barrier_semaphore()
    for k in range(1, N):
        pl.semaphore_signal(barrier, inc=1, device_id={"ep": (me + k) % N}, device_id_type=pl.DeviceIdType.MESH)
    pl.semaphore_wait(barrier, N - 1)
    for k in range(1, N):
        send(info, rows(infos, me * 16, 16), is_, ir, (me + k) % N)
    wait(xbuf, NS * T, xsem)
    own_out(0)
    own_out(1)
    infos[pl.ds(pl.multiple_of(me * 16, 16), 16), :] = info[...]

    def shared_step(c, _):
        base = wait_item(c)
        lhs = jnp.concatenate([xr(2 * c, me)[...], xr(2 * c + 1, me)[...]], axis=1)
        for t in range(NT):
            r = dot(lhs, ld(w, base + t * KC, KC))
            at = pl.ds(t * ROWS, T)
            acc[at, :] = jnp.where(c > 0, acc[at, :], 0.0) + r
        start_item(c + NSLOT)

        @pl.when(c == 4)
        def _():
            tick(jnp.int32(0))
        return 0

    lax.fori_loop(0, NC, shared_step, 0)

    def act(g, u):
        return (g * (0.5 * jnp.tanh(0.5 * g) + 0.5) * u).astype(bf16)

    def hidden(g0, n, put):
        for t in range(5):
            put(t, act(ld(acc, t * ROWS + g0, n), ld(acc, (6 + t) * ROWS + g0, n)), W)
        v = ld(acc, 5 * ROWS + g0, n)
        put(5, act(v[:, :128], v[:, 128:]), 128)

    def put_shared(t, v, n):
        hsh[:, t * W:t * W + n] = v

    hidden(0, T, put_shared)
    tick(jnp.int32(1))

    wait(infos, 7 * 16, ir)
    wait(infos, 7 * 16, is_)
    base_row = (me * R).astype(f32)

    def tables(s, _):
        v = infos[pl.ds(pl.multiple_of(s * 16, 16), 16), :]
        rid = lax.broadcasted_iota(jnp.int32, (R, T), 0).astype(f32) + base_row
        m = rid == v[0:1, :]
        for j in range(1, 8):
            m = m | (rid == v[j:j + 1, :])
        dm[pl.ds(pl.multiple_of(s * R, 16), R), :] = jnp.where(m, 1.0, 0.0).astype(bf16)
        vt = v.T
        cid = lax.broadcasted_iota(jnp.int32, (T, R), 1).astype(f32) + base_row
        o = jnp.zeros((T, R), f32)
        for j in range(8):
            o = o + jnp.where(cid == vt[:, j:j + 1], vt[:, 8 + j:9 + j], 0.0)
        cm[pl.ds(pl.multiple_of(s * T, 16), T), :] = o.astype(bf16)
        return 0

    lax.fori_loop(0, N, tables, 0)
    tick(jnp.int32(2))

    def chunk(c, _):
        for h in range(2):
            wait(xbuf, 4 * T, sb_r.at[2 * c + h])
        for h in range(2):
            for p in range(4):
                r = [dot(dm[(2 * p + q) * R:(2 * p + q + 1) * R, :], xr(2 * c + h, 2 * p + q)[...]) for q in range(2)]
                for e in range(EL):
                    z[h * ROWS + e * EM + p * 80:h * ROWS + e * EM + p * 80 + 80, :] = jnp.concatenate(
                        [r[0][e * SL:(e + 1) * SL], r[1][e * SL:(e + 1) * SL]], axis=0).astype(bf16)

        def one(e, _):
            i = NC + c * EL + e
            @pl.when(e == 0)
            def _():
                tick(2 * c + 3)

            @pl.when(e == 4)
            def _():
                tick(2 * c + 4)
            base = wait_item(i)
            lhs = jnp.concatenate([ld(z, e * EM, EM), ld(z, ROWS + e * EM, EM)], axis=1)
            for t in range(NT):
                r = dot(lhs, ld(w, base + t * KC, KC))
                at = pl.ds(pl.multiple_of(t * ROWS + e * EM, 8), EM)
                acc[at, :] = jnp.where(c > 0, acc[at, :], 0.0) + r
            start_item(i + NSLOT)
            return 0

        lax.fori_loop(0, EL, one, 0)
        return 0

    lax.fori_loop(0, NC, chunk, 0)

    for s in range(NS):
        wait(xbuf, 7 * T, ag_s.at[s])
    for dev in (dx, dy, ds):
        pl.semaphore_signal(ready, inc=1, device_id={"ep": dev}, device_id_type=pl.DeviceIdType.MESH)

    def hid(e, _):
        def put(t, v, n):
            xbuf[pl.ds(pl.multiple_of(t * ROWS + e * EM, 16), EM), 0:n] = v
        hidden(e * EM, EM, put)
        return 0

    lax.fori_loop(0, EL, hid, 0)

    def chip(q):
        return ((mx + q // 2) % 2) * 2 + (my + q % 2) % 2

    def q_at(c, q, h, r0=0, n=T):
        return pl.ds(pl.multiple_of(((c * 4 + q) * 2 + h) * T + r0, 8), n)

    def combine(c):
        slot = c % 2

        @pl.when(c >= 2)
        def _():
            wait(ssend, 2048, sib_s.at[slot])
        for q in range(4):
            s = chip(q) * 2 + (1 - mc)
            cw = ld(cm, s * T, T)
            for h in range(2):
                r = dot(cw, ld(z, h * ROWS + s * R, R))
                ssend[pl.ds(pl.multiple_of(slot * 2048 + (q * 2 + h) * T, T), T), :] = r.astype(bf16)

        @pl.when(c == 0)
        def _():
            pl.semaphore_wait(ready, 3)

        @pl.when(c >= 2)
        def _():
            pl.semaphore_wait(credit, 1)
        for q in range(4):
            s = chip(q) * 2 + mc
            cw = ld(cm, s * T, T)
            for h in range(2):
                acc[q_at(c, q, h), :] = dot(cw, ld(z, h * ROWS + s * R, R))
        send(rows(ssend, slot * 2048, 2048), rows(xbuf, SIBR + slot * 2048, 2048), sib_s.at[slot], sib_r.at[slot], ds)

    def pairs(c):
        slot = c % 2
        wait(xbuf, 2048, sib_r.at[slot])

        @pl.when(c >= 2)
        def _():
            wait(xbuf, 512, s1_s.at[slot])
        sib = SIBR + slot * 2048
        for q in range(4):
            for h in range(2):
                r = acc[q_at(c, q, h), :] + ld(xbuf, sib + (q * 2 + h) * T, T).astype(f32)
                if q < 3:
                    acc[q_at(c, q, h), :] = r
                else:
                    for k in range(2):
                        xbuf[pl.ds(pl.multiple_of(S1S + slot * 512 + (k * 2 + h) * 128, 128), 128), :] = (
                            r[k * 128:(k + 1) * 128].astype(bf16))

        @pl.when(c < NC - 2)
        def _():
            pl.semaphore_signal(credit, inc=1, device_id={"ep": ds}, device_id_type=pl.DeviceIdType.MESH)
        for k, dev in ((0, dx), (1, dy)):
            send(rows(xbuf, S1S + slot * 512 + k * 256, 256), rows(xbuf, S1R + c * 512 + k * 256, 256),
                 s1_s.at[slot], s1_r.at[c], dev)

    def paths(c):
        slot = c % 2
        wait(xbuf, 512, s1_r.at[c])

        @pl.when(c >= 2)
        def _():
            wait(xbuf, 1024, s2_s.at[slot])
        got = S1R + c * 512
        for h in range(2):
            yn = acc[q_at(c, 1, h), :]
            yn = jnp.concatenate([yn[:128] + ld(xbuf, got + h * 128, 128).astype(f32), yn[128:]], axis=0)
            xn = acc[q_at(c, 2, h), :]
            xn = jnp.concatenate([xn[:128], xn[128:] + ld(xbuf, got + 256 + h * 128, 128).astype(f32)], axis=0)
            for k, v in ((0, xn), (1, yn)):
                dm[pl.ds(pl.multiple_of(slot * 1024 + (k * 2 + h) * T, T), T), :] = v.astype(bf16)
        for k, dev in ((0, dx), (1, dy)):
            send(rows(dm, slot * 1024 + k * 512, 512), rows(xbuf, S2R + c * 1024 + k * 512, 512),
                 s2_s.at[slot], s2_r.at[c], dev)

    def result(c):
        wait(xbuf, 1024, s2_r.at[c])

        @pl.when(c >= 1)
        def _():
            wait(dm, 512, ysem)
        got = S2R + c * 1024
        for h in range(2):
            r = acc[q_at(c, 0, h), :] + ld(xbuf, got + h * T, T).astype(f32) + ld(xbuf, got + 512 + h * T, T).astype(f32)
            r = r + ld(acc, SHR + (c * 2 + h) * T, T)
            dm[YST + h * T:YST + (h + 1) * T, :] = r.astype(bf16)
        for h in range(2):
            pltpu.make_async_copy(
                dm.at[pl.ds(YST + h * T, T)],
                y.at[:, pl.ds(pl.multiple_of(c * KC + h * W, W), W)], ysem).start()

    def column(c, _):
        @pl.when((c >= 1) & (c < NC + 1))
        def _():
            pairs(c - 1)

        @pl.when(c < NC)
        def _():
            i = ITEMS1 + c * PER2

            def pair(j, _):
                base = wait_item(i + j)
                for h in range(2):
                    r = []
                    for ee in range(2):
                        e = j * 2 + ee
                        lhs = jnp.concatenate(
                            [ld(xbuf, t * ROWS + e * EM, EM) for t in range(5)]
                            + [xbuf[pl.ds(pl.multiple_of(5 * ROWS + e * EM, 16), EM), 0:128]], axis=1)
                        r.append(dot(lhs, ld(w, base + (ee * 2 + h) * FF, FF)))
                    for s in range(N):
                        z[pl.ds(pl.multiple_of(h * ROWS + s * R + j * 80, 16), 80), :] = jnp.concatenate(
                            [r[0][s * SL:(s + 1) * SL], r[1][s * SL:(s + 1) * SL]], axis=0).astype(bf16)
                start_item(i + j + NSLOT)

                @pl.when((j == 1) & (c >= 2))
                def _():
                    paths(c - 2)
                return 0

            lax.fori_loop(0, 4, pair, 0)
            base = wait_item(i + 4, SLOT // 2)
            for h in range(2):
                acc[pl.ds(pl.multiple_of(SHR + (c * 2 + h) * T, 8), T), :] = dot(hsh[...], ld(w, base + h * FF, FF))
            start_item(i + 4 + NSLOT)
            combine(c)

        @pl.when((c >= NC) & (c < NC + 2))
        def _():
            paths(c - 2)

        @pl.when(c >= 3)
        def _():
            result(c - 3)
        return 0

    lax.fori_loop(0, NC + 3, column, 0)
    wait(dm, 512, ysem)
    for slot in range(2):
        wait(ssend, 2048, sib_s.at[slot])
        wait(xbuf, 512, s1_s.at[slot])
        wait(xbuf, 1024, s2_s.at[slot])


def solution(mesh):
    def step(x, expert, slot, gate, w_gate, w_up, w_down, s_gate, s_up, s_down):
        x = x.reshape(T, D)
        code = jnp.where(slot < SL, expert * SL + slot, -1).reshape(T, 8).astype(f32)
        g = gate.reshape(T, 8).astype(bf16).astype(f32)
        info = jnp.concatenate([code.T, g.T], axis=0)
        hbm, vmem = pl.BlockSpec(memory_space=pl.ANY), pl.BlockSpec(memory_space=pltpu.VMEM)
        dma = pltpu.SemaphoreType.DMA
        y = pl.pallas_call(
            kernel,
            out_shape=jax.ShapeDtypeStruct((T, D), bf16),
            in_specs=[hbm, vmem] + [hbm] * 6,
            out_specs=hbm,
            scratch_shapes=[
                pltpu.VMEM((XROWS, W), bf16),
                pltpu.VMEM((NT * ROWS, W), f32),
                pltpu.VMEM((NSLOT * SLOT, W), bf16),
                pltpu.VMEM((2 * ROWS, W), bf16),
                pltpu.VMEM((N * R, T), bf16),
                pltpu.VMEM((N * T, R), bf16),
                pltpu.VMEM((T, FF), bf16),
                pltpu.VMEM((2 * 2048, W), bf16),
                pltpu.VMEM((N * 16, T), f32),
                dma((NSLOT,)), dma, dma, dma,
                dma((NS,)), dma((NS,)), dma((NS,)), dma((NS,)),
                dma((2,)), dma((2,)), dma((2,)), dma((NC,)), dma((2,)), dma((NC,)), dma,
                pltpu.SemaphoreType.REGULAR, pltpu.SemaphoreType.REGULAR,
            ],
            compiler_params=pltpu.CompilerParams(
                collective_id=0, has_side_effects=True, vmem_limit_bytes=67043328),
        )(x, info, w_gate, w_up, w_down, s_gate, s_up, s_down)
        return y.reshape(1, 1, T, D)

    tok, exp = P("dp", "ep", None, None), P("ep", None, None)
    whole = P(None, None)
    return jax.shard_map(
        step, mesh=mesh,
        in_specs=(tok, tok, tok, tok, exp, exp, exp, whole, whole, whole),
        out_specs=tok, check_vma=False)
```

```python
import functools

import jax
import jax.numpy as jnp
from jax import lax
from jax.experimental import pallas as pl
from jax.experimental.pallas import tpu as pltpu
from jax.sharding import PartitionSpec as P

N = 8
T = 256
D = 4096
FF = 1408
EL = 8
SL = 40
R = EL * SL
EM = N * SL
ROWS = EL * EM
W = 256
KC = 512
NC = D // KC
NS = D // W
NT = 2 * FF // W
KT = 6
SLOT = 5632
NSLOT = 4
ITEMS1 = NC + NC * EL
LAG = 4
ITEMS = ITEMS1 + 3 * (NS + LAG)
RING = 4

S1R = KT * ROWS
S2R = S1R + NS * T
SIBR = S2R + NS * 2 * T
S1S = SIBR + RING * 4 * T
XROWS = S1S + RING * T
YST = RING * 2 * T
SHR = NS * 4 * T

f32, bf16 = jnp.float32, jnp.bfloat16


def dot(a, b):
    return jnp.dot(a, b, preferred_element_type=f32)


def kernel(x, expert, slot, gate, wg, wu, wd, sg, su, sd, y, xbuf, acc, w, z, dm, cm, hsh, ssend, infos, info,
           wsem, xsem, is_, ir, ag_s, xy_r, dg_r, sb_r, sib_s, sib_r, s1_s, s1_r, s2_s, s2_r, ysem, credit, ready):
    me = lax.axis_index("ep")
    mx, my, mc = me // 4, (me // 2) % 2, me % 2
    dx = (1 - mx) * 4 + my * 2 + mc
    dy = mx * 4 + (1 - my) * 2 + mc
    dd = (1 - mx) * 4 + (1 - my) * 2 + mc
    ds = mx * 4 + my * 2 + (1 - mc)

    def rows(ref, start, n):
        return ref.at[pl.ds(pl.multiple_of(start, 8), n)]

    def ld(ref, start, n):
        return ref[pl.ds(pl.multiple_of(start, 8), n), :]

    def send(src, dst, ss, rs, dev):
        pltpu.make_async_remote_copy(
            src_ref=src, dst_ref=dst, send_sem=ss, recv_sem=rs,
            device_id={"ep": dev}, device_id_type=pl.DeviceIdType.MESH).start()

    def wait(ref, n, sem, name="wait"):
        with jax.named_scope(name):
            v = ref.at[pl.ds(0, n)]
            pltpu.make_async_copy(v, v, sem).wait()

    def start_item(i):
        slot = i % NSLOT
        base = slot * SLOT
        sem = wsem.at[slot]

        def first(g, u, c):
            def put(src, c0, n, t, l0):
                pltpu.make_async_copy(
                    src.at[pl.ds(pl.multiple_of(c * KC, KC), KC), pl.ds(c0, n)],
                    w.at[pl.ds(pl.multiple_of(base + t * KC, KC), KC), pl.ds(l0, n)], sem).start()
            for t in range(5):
                put(g, t * W, W, t, 0)
            put(g, 5 * W, 128, 5, 0)
            put(u, 5 * W, 128, 5, 128)
            for t in range(5):
                put(u, t * W, W, 6 + t, 0)

        @pl.when(i < NC)
        def _():
            first(sg, su, i)

        @pl.when((i >= NC) & (i < ITEMS1))
        def _():
            k = i - NC
            first(wg.at[k % EL], wu.at[k % EL], k // EL)

        @pl.when((i >= ITEMS1) & (i < ITEMS))
        def _():
            k = i - ITEMS1
            c, j = k // 3, k % 3

            def put(src, c, t):
                pltpu.make_async_copy(
                    src.at[:, pl.ds(pl.multiple_of(c * W, W), W)], rows(w, base + t * FF, FF), sem).start()

            @pl.when((j < 2) & (c < NS))
            def _():
                for t in range(4):
                    put(wd.at[j * 4 + t], c, t)

            @pl.when((j == 2) & (c >= LAG))
            def _():
                put(sd, c - LAG, 0)

    def wait_item(i, n=SLOT):
        wait(w, n, wsem.at[i % NSLOT], "w_weights")
        return (i % NSLOT) * SLOT

    def xr(s, src, r0=0, n=T):
        return rows(xbuf, (s * N + src) * T + r0, n)

    def own_out(s):
        for dev, sem in ((dx, xy_r), (dy, xy_r), (ds, sb_r)):
            send(xr(s, me), xr(s, me), ag_s.at[s], sem.at[s], dev)

    def pass_on(k):
        wait(xbuf, 2 * T, xy_r.at[k], "w_xy")
        send(xr(k, dx, 0, 128), xr(k, dx, 0, 128), ag_s.at[k], dg_r.at[k], dy)
        send(xr(k, dy, 128, 128), xr(k, dy, 128, 128), ag_s.at[k], dg_r.at[k], dx)
        send(xr(k, dx), xr(k, dx), ag_s.at[k], sb_r.at[k], ds)
        send(xr(k, dy), xr(k, dy), ag_s.at[k], sb_r.at[k], ds)

    def diagonal(k):
        wait(xbuf, T, dg_r.at[k], "w_diag")
        send(xr(k, dd), xr(k, dd), ag_s.at[k], sb_r.at[k], ds)

    def tick(k):
        @pl.when(k < NS)
        def _():
            pass_on(k)

        @pl.when(k + 2 < NS)
        def _():
            own_out(k + 2)

        @pl.when(k <= NS)
        def _():
            diagonal(k - 1)

    for s in range(NS):
        pltpu.make_async_copy(x.at[:, pl.ds(s * W, W)], xr(s, me), xsem).start()
    for i in range(NSLOT):
        start_item(jnp.int32(i))
    code = jnp.where(slot[...] < SL, expert[...] * SL + slot[...], -1).astype(f32)
    mine = jnp.concatenate([code, gate[...].astype(bf16).astype(f32)], axis=1).T
    info[...] = mine
    infos[pl.ds(pl.multiple_of(me * 16, 16), 16), :] = mine
    barrier = pltpu.get_barrier_semaphore()
    for k in range(1, N):
        pl.semaphore_signal(barrier, inc=1, device_id={"ep": (me + k) % N}, device_id_type=pl.DeviceIdType.MESH)
    with jax.named_scope("w_barrier"):
        pl.semaphore_wait(barrier, N - 1)
    wait(xbuf, NS * T, xsem)
    own_out(0)
    for k in range(1, N):
        send(info, rows(infos, me * 16, 16), is_, ir, (me + k) % N)

    def shared_step(p, _):
        base = [wait_item(2 * p + k) for k in range(2)]
        for k in range(2):
            c = 2 * p + k
            lhs = jnp.concatenate([xr(2 * c, me)[...], xr(2 * c + 1, me)[...]], axis=1)
            for t in range(NT):
                r = dot(lhs, ld(w, base[k] + t * KC, KC))
                at = pl.ds(t * ROWS, T)
                acc[at, :] = (jnp.where(p > 0, acc[at, :], 0.0) if k == 0 else acc[at, :]) + r
        for k in range(2):
            start_item(2 * p + k + NSLOT)

        @pl.when(p == 0)
        def _():
            own_out(1)

        @pl.when(p == 1)
        def _():
            pass_on(0)
            own_out(2)
        return 0

    with jax.named_scope("shared"):
        lax.fori_loop(0, NC // 2, shared_step, 0)

    def act(g, u):
        return (g * (0.5 * jnp.tanh(0.5 * g) + 0.5) * u).astype(bf16)

    pass_on(1)
    own_out(3)
    diagonal(0)
    for t in range(5):
        hsh[:, t * W:t * W + W] = act(acc[t * ROWS:t * ROWS + T, :], acc[(6 + t) * ROWS:(6 + t) * ROWS + T, :])
    v = acc[5 * ROWS:5 * ROWS + T, :]
    hsh[:, 5 * W:] = act(v[:, :128], v[:, 128:])

    wait(infos, 7 * 16, ir)
    wait(infos, 7 * 16, is_)
    base_row = (me * R).astype(f32)

    def tables(s, _):
        v = infos[pl.ds(pl.multiple_of(s * 16, 16), 16), :]
        for k in range(0, R, 128):
            part = []
            for k2 in range(k, min(k + 128, R), 64):
                rid = lax.broadcasted_iota(jnp.int32, (64, T), 0).astype(f32) + (base_row + k2)
                o, g = jnp.zeros((64, T), f32), jnp.zeros((64, T), f32)
                for j in range(8):
                    m = rid == v[j:j + 1, :]
                    o = jnp.where(m, 1.0, o)
                    g = jnp.where(m, v[8 + j:9 + j, :], g)
                dm[pl.ds(pl.multiple_of(s * R + k2, 16), 64), :] = o.astype(bf16)
                part.append(g)
            g = jnp.concatenate(part, axis=0).T
            cm[pl.ds(pl.multiple_of(s * T, 16), T), k:k + g.shape[1]] = g.astype(bf16)
        return 0

    with jax.named_scope("tables"):
        lax.fori_loop(0, N, tables, 0)
    diagonal(1)
    pass_on(2)
    own_out(4)

    def chunk(c, last):
        for h in range(2):
            wait(xbuf, 4 * T, sb_r.at[2 * c + h], "w_sib_x")
        for h in range(2):
            for p in range(4):
                r = [dot(dm[(2 * p + q) * R:(2 * p + q + 1) * R, :], xr(2 * c + h, 2 * p + q)[...]) for q in range(2)]
                for e in range(EL):
                    z[h * ROWS + e * EM + p * 80:h * ROWS + e * EM + p * 80 + 80, :] = jnp.concatenate(
                        [r[0][e * SL:(e + 1) * SL], r[1][e * SL:(e + 1) * SL]], axis=0).astype(bf16)
        if last:
            for s in range(NS):
                wait(xbuf, 7 * T, ag_s.at[s], "w_sent")
            for dev in (dx, dy, ds):
                pl.semaphore_signal(ready, inc=1, device_id={"ep": dev}, device_id_type=pl.DeviceIdType.MESH)

        def two(p, _):
            i = NC + c * EL + 2 * p
            if not last:
                @pl.when(p == 0)
                def _():
                    tick(2 * c + 3)

                @pl.when(p == 2)
                def _():
                    tick(2 * c + 4)
            base = [wait_item(i + k) for k in range(2)]
            for k in range(2):
                e = 2 * p + k
                lhs = jnp.concatenate([ld(z, e * EM, EM), ld(z, ROWS + e * EM, EM)], axis=1)

                def total(t):
                    at = pl.ds(pl.multiple_of(t * ROWS + e * EM, 8), EM)
                    r = dot(lhs, ld(w, base[k] + t * KC, KC))
                    return at, (acc[at, :] if last else jnp.where(c > 0, acc[at, :], 0.0)) + r

                def put(t, v, n):
                    xbuf[pl.ds(pl.multiple_of(t * ROWS + e * EM, 16), EM), 0:n] = v

                if last:
                    for t in range(5):
                        put(t, act(total(t)[1], total(6 + t)[1]), W)
                    v = total(5)[1]
                    put(5, act(v[:, :128], v[:, 128:]), 128)
                else:
                    for t in range(NT):
                        at, r = total(t)
                        acc[at, :] = r
            for k in range(2):
                start_item(i + k + NSLOT)
            return 0

        with jax.named_scope("experts"):
            lax.fori_loop(0, EL // 2, two, 0)

    def chunk_step(c, _):
        chunk(c, False)
        return 0

    with jax.named_scope("phase1"):
        lax.fori_loop(0, NC - 1, chunk_step, 0)
    with jax.named_scope("phase1_last"):
        chunk(NC - 1, True)

    def chip(q):
        return ((mx + q // 2) % 2) * 2 + (my + q % 2) % 2

    def q_at(c, q):
        return pl.ds(pl.multiple_of((c * 4 + q) * T, 8), T)

    def part(ref, start, n=T):
        return ref[pl.ds(pl.multiple_of(start, 16), n), :].astype(f32)

    def combine(c):
        slot = c % RING

        @pl.when(c >= RING)
        def _():
            wait(ssend, 4 * T, sib_s.at[slot], "w_sib_s")
        for q in range(4):
            s = chip(q) * 2 + (1 - mc)
            r = dot(ld(cm, s * T, T), ld(z, s * R, R))
            ssend[pl.ds(pl.multiple_of((slot * 4 + q) * T, T), T), :] = r.astype(bf16)

        @pl.when(c == 0)
        def _():
            with jax.named_scope("w_ready"):
                pl.semaphore_wait(ready, 3)

        @pl.when(c >= RING)
        def _():
            with jax.named_scope("w_credit"):
                pl.semaphore_wait(credit, 1)
        for q in range(4):
            s = chip(q) * 2 + mc
            acc[q_at(c, q), :] = dot(ld(cm, s * T, T), ld(z, s * R, R))
        send(rows(ssend, slot * 4 * T, 4 * T), rows(xbuf, SIBR + slot * 4 * T, 4 * T), sib_s.at[slot], sib_r.at[slot], ds)

    def pairs(c):
        slot = c % RING
        wait(xbuf, 4 * T, sib_r.at[slot], "w_sib_r")

        @pl.when(c >= RING)
        def _():
            wait(xbuf, T, s1_s.at[slot], "w_s1_s")
        sib = SIBR + slot * 4 * T
        r = acc[q_at(c, 3), :] + part(xbuf, sib + 3 * T)
        xbuf[pl.ds(pl.multiple_of(S1S + slot * T, T), T), :] = r.astype(bf16)
        for q in range(3):
            acc[q_at(c, q), :] += part(xbuf, sib + q * T)

        @pl.when(c < NS - RING)
        def _():
            pl.semaphore_signal(credit, inc=1, device_id={"ep": ds}, device_id_type=pl.DeviceIdType.MESH)
        for k, dev in ((0, dx), (1, dy)):
            send(rows(xbuf, S1S + slot * T + k * 128, 128), rows(xbuf, S1R + c * T + k * 128, 128),
                 s1_s.at[slot], s1_r.at[c], dev)

    def paths(c):
        slot = c % RING
        wait(xbuf, T, s1_r.at[c], "w_s1_r")

        @pl.when(c >= RING)
        def _():
            wait(xbuf, 2 * T, s2_s.at[slot], "w_s2_s")
        got = S1R + c * T
        yn, xn = acc[q_at(c, 1), :], acc[q_at(c, 2), :]
        yn = jnp.concatenate([yn[:128] + part(xbuf, got, 128), yn[128:]], axis=0)
        xn = jnp.concatenate([xn[:128], xn[128:] + part(xbuf, got + 128, 128)], axis=0)
        for k, v in ((0, xn), (1, yn)):
            dm[pl.ds(pl.multiple_of((slot * 2 + k) * T, T), T), :] = v.astype(bf16)
        for k, dev in ((0, dx), (1, dy)):
            send(rows(dm, (slot * 2 + k) * T, T), rows(xbuf, S2R + (c * 2 + k) * T, T), s2_s.at[slot], s2_r.at[c], dev)

    def result(c):
        wait(xbuf, 2 * T, s2_r.at[c], "w_s2_r")
        slot = c % 2

        @pl.when(c >= 2)
        def _():
            wait(dm, T, ysem.at[slot], "w_y")
        got = S2R + c * 2 * T
        r = acc[q_at(c, 0), :] + part(xbuf, got) + part(xbuf, got + T) + ld(acc, SHR + c * T, T)
        at = pl.ds(pl.multiple_of(YST + slot * T, T), T)
        dm[at, :] = r.astype(bf16)
        pltpu.make_async_copy(dm.at[at], y.at[:, pl.ds(pl.multiple_of(c * W, W), W)], ysem.at[slot]).start()

    def four(c, j):
        i = ITEMS1 + c * 3 + j
        base = wait_item(i)
        for k in range(0, 4, 2):
            r = []
            for ee in (k, k + 1):
                e = j * 4 + ee
                lhs = jnp.concatenate(
                    [ld(xbuf, t * ROWS + e * EM, EM) for t in range(5)]
                    + [xbuf[5 * ROWS + e * EM:5 * ROWS + (e + 1) * EM, 0:128]], axis=1)
                r.append(dot(lhs, ld(w, base + ee * FF, FF)))
            for s in range(N):
                z[s * R + (j * 4 + k) * SL:s * R + (j * 4 + k) * SL + 80, :] = jnp.concatenate(
                    [r[0][s * SL:(s + 1) * SL], r[1][s * SL:(s + 1) * SL]], axis=0).astype(bf16)

    def column(c, _):
        i = ITEMS1 + c * 3

        @pl.when(c < NS)
        def _():
            with jax.named_scope("down"):
                four(c, 0)
        start_item(i + NSLOT)

        @pl.when((c >= 1) & (c < NS + 1))
        def _():
            pairs(c - 1)

        @pl.when(c < NS)
        def _():
            with jax.named_scope("down"):
                four(c, 1)
        start_item(i + 1 + NSLOT)

        @pl.when((c >= 2) & (c < NS + 2))
        def _():
            paths(c - 2)

        @pl.when(c < NS)
        def _():
            with jax.named_scope("combine"):
                combine(c)

        @pl.when(c >= LAG)
        def _():
            base = wait_item(i + 2, FF)
            acc[pl.ds(pl.multiple_of(SHR + (c - LAG) * T, 8), T), :] = dot(hsh[...], ld(w, base, FF))
            result(c - LAG)
        start_item(i + 2 + NSLOT)
        return 0

    with jax.named_scope("phase2"):
        lax.fori_loop(0, NS + LAG, column, 0)
    for slot in range(2):
        wait(dm, T, ysem.at[slot])
    for slot in range(RING):
        wait(ssend, 4 * T, sib_s.at[slot])
        wait(xbuf, T, s1_s.at[slot])
        wait(xbuf, 2 * T, s2_s.at[slot])


def solution(mesh):
    def step(x, expert, slot, gate, w_gate, w_up, w_down, s_gate, s_up, s_down):
        x = x.reshape(T, D)
        expert, slot, gate = (v.reshape(T, 8) for v in (expert, slot, gate))
        hbm, vmem = pl.BlockSpec(memory_space=pl.ANY), pl.BlockSpec(memory_space=pltpu.VMEM)
        dma = pltpu.SemaphoreType.DMA
        y = pl.pallas_call(
            kernel,
            out_shape=jax.ShapeDtypeStruct((T, D), bf16),
            in_specs=[hbm] + [vmem] * 3 + [hbm] * 6,
            out_specs=hbm,
            scratch_shapes=[
                pltpu.VMEM((XROWS, W), bf16),
                pltpu.VMEM((NT * ROWS, W), f32),
                pltpu.VMEM((NSLOT * SLOT, W), bf16),
                pltpu.VMEM((2 * ROWS, W), bf16),
                pltpu.VMEM((N * R, T), bf16),
                pltpu.VMEM((N * T, R), bf16),
                pltpu.VMEM((T, FF), bf16),
                pltpu.VMEM((RING * 4 * T, W), bf16),
                pltpu.VMEM((N * 16, T), f32),
                pltpu.VMEM((16, T), f32),
                dma((NSLOT,)), dma, dma, dma,
                dma((NS,)), dma((NS,)), dma((NS,)), dma((NS,)),
                dma((RING,)), dma((RING,)), dma((RING,)), dma((NS,)), dma((RING,)), dma((NS,)), dma((2,)),
                pltpu.SemaphoreType.REGULAR, pltpu.SemaphoreType.REGULAR,
            ],
            compiler_params=pltpu.CompilerParams(
                collective_id=0, has_side_effects=True, vmem_limit_bytes=67043328),
        )(x, expert, slot, gate, w_gate, w_up, w_down, s_gate, s_up, s_down)
        return y.reshape(1, 1, T, D)

    tok, exp = P("dp", "ep", None, None), P("ep", None, None)
    whole = P(None, None)
    return jax.shard_map(
        step, mesh=mesh,
        in_specs=(tok, tok, tok, tok, exp, exp, exp, whole, whole, whole),
        out_specs=tok, check_vma=False)
```
